32 devices in a mesh: ctx: 8 (over z, x), dp: 4 (over y, core).
Axes of the slice: x: 2, y: 2, z: 4, core: 2. Of those that a mesh axis runs over, the one named last changes fastest.
Arguments:
- head_input: bfloat16 [8192, 4096], P(('dp', 'ctx')), parts along dimension 0, may hold values from -6 to 6
- gate_input: bfloat16 [8192, 4096], P(('dp', 'ctx')), parts along dimension 0, may hold values from -6 to 6
- write_vector: bfloat16 [8192, 128], P(('dp', 'ctx')), parts along dimension 0, may hold values from -2.5 to 2.5
- read_vector: bfloat16 [8192, 128], P(('dp', 'ctx')), parts along dimension 0, may hold values from -2.5 to 2.5
- increment_preactivation: bfloat16 [8192, 64], P(('dp', 'ctx')), parts along dimension 0, may hold values from -2 to 8
- step_bias: float32 [64], replicated, may hold values from -1 to 0.5
- decay_log: float32 [64], replicated, may hold values from -9.3 to -2.3
- skip_gain: float32 [64], replicated, may hold values from 0.5 to 1.5
- norm_weight: float32 [4096], replicated, may hold values from 0.5 to 1.5
- doc_starts: int32 [64], P(('dp', 'ctx')), parts along dimension 0, may hold values from 0 to 1, as said below
- block_order: int32 [64], P(('dp', 'ctx')), parts along dimension 0, may hold values from 0 to 15, as said below
Outputs:
- packed_out: bfloat16 [8192, 4096], P(('dp', 'ctx')), parts along dimension 0
The draws below stay inside these ranges and needn't reach their ends.
There are 4 independent parts, one for each index of `dp`. The reference program is written for one: setup_inputs(seed, part) draws one part's arguments, and reference() takes and returns one part's arrays. A program takes and returns all parts, laid end to end along the dimension named above; an argument that names none is the same for every part. Nothing has to cross between parts.
Inputs may be any that keep to these rules, and one draw needn't show every extreme that they name: `doc_starts`: block 0 starts a document; no document is longer than 128 blocks. `block_order`: a permutation of the block indices that keeps each document's blocks together and in their order.
All inputs are finite; a program needn't handle non-finite values.
Results may differ from the reference program's by a relative error of at most 0.0085.
Values may be sent and summed in bfloat16 or wider, within the bound.
A program may use at most 128 MiB of HBM per device.

```python
import math
import jax
import jax.numpy as jnp
from jax import lax

HEADS = 64
HEAD_DIM = 64
STATE = 128
GROUP = 128
DOC_MOST = 128
JOINED_TERMS = 2048


def doc_tables(key):
    key_baseline = jax.random.fold_in(key, 7)
    key_start, key_rank, key_extra = jax.random.split(key_baseline, 3)
    block_count = JOINED_TERMS // GROUP
    positions = jnp.arange(block_count, dtype=jnp.int32)
    chosen = jax.random.randint(key_start, (block_count,), 0, 64) == 0
    extra_at = jax.random.randint(key_extra, (4,), 1, block_count)
    hit_extra = jnp.any(positions[:, None] == extra_at[None, :], axis=1)
    forced = jnp.logical_or(positions % DOC_MOST == 0, hit_extra)
    starts = jnp.logical_or(chosen, forced).astype(jnp.int32)
    segment_number = jnp.cumsum(starts) - 1
    ranks = jax.random.randint(key_rank, (block_count,), 0, 1 << 20)
    priority = ranks[segment_number] * block_count + positions
    permuted = jnp.argsort(priority, stable=True).astype(jnp.int32)
    return (starts, permuted)


def draw_doc_starts(key, part):
    return doc_tables(key)[0]


def draw_block_order(key, part):
    return doc_tables(key)[1]


def draw_increment_preactivation(key, part):
    key_baseline = jax.random.fold_in(key, 11)
    key_value_product, lookup_jump = jax.random.split(key_baseline)
    spike_series = (jax.random.randint(lookup_jump, (JOINED_TERMS, 1), 0, 64) == 0).astype(jnp.float32)
    payload_reference_level = jnp.clip(0.5 * jax.random.normal(key_value_product, (JOINED_TERMS, HEADS), jnp.float32), -2.0, 2.0)
    return (payload_reference_level + 6.0 * spike_series).astype(jnp.bfloat16)


def draw_decay_log(key, part):
    key_baseline = jax.random.fold_in(key, 13)
    return jax.random.uniform(key_baseline, (HEADS,), jnp.float32, math.log(0.0003), math.log(0.1))


def levels(own_key, dims, shards, low, largest):
    gain = 1.0
    for axis_at, blocks in shards:
        steps = jax.random.uniform(jax.random.fold_in(jax.random.fold_in(own_key, 6), axis_at), (blocks,), jnp.float32, low / len(shards), largest / len(shards))
        gain = gain * jnp.repeat(jnp.exp(steps), dims[axis_at] // blocks).reshape((-1,) + (1,) * (len(dims) - 1 - axis_at))
    return gain


def noise(stream_key, extent, scale, reach, cuts=(), kind=jnp.bfloat16):
    entries = scale * jax.random.normal(stream_key, extent, jnp.float32)
    if cuts:
        entries = entries * levels(stream_key, extent, cuts, -0.22, 0.18)
    return jnp.clip(entries, -reach, reach).astype(kind)


def setup_inputs(seed: int = 0, part: int = 0) -> dict:
    streams_of = jax.random.split(jax.random.key(seed), 12)
    part_keys = jax.random.split(jax.random.fold_in(streams_of[11], part), 12)
    return {
        "head_input": noise(part_keys[0], (JOINED_TERMS, HEADS * HEAD_DIM), 1.0, 6.0, ((0, 8),)),
        "gate_input": noise(part_keys[1], (JOINED_TERMS, HEADS * HEAD_DIM), 1.0, 6.0, ((0, 8),)),
        "write_vector": noise(part_keys[2], (JOINED_TERMS, STATE), 0.3, 2.5, ((0, 8),)),
        "read_vector": noise(part_keys[3], (JOINED_TERMS, STATE), 0.3, 2.5, ((0, 8),)),
        "increment_preactivation": draw_increment_preactivation(jax.random.fold_in(jax.random.fold_in(streams_of[11], part), 71), part),
        "step_bias": jnp.clip(jax.random.uniform(streams_of[5], (HEADS,), jnp.float32, -1.0, 0.5), -1.0, 0.5),
        "decay_log": draw_decay_log(jax.random.fold_in(streams_of[11], 71), part),
        "skip_gain": jnp.clip(jax.random.uniform(streams_of[7], (HEADS,), jnp.float32, 0.5, 1.5), 0.5, 1.5),
        "norm_weight": jnp.clip(1.0 + 0.1 * jax.random.normal(streams_of[8], (HEADS * HEAD_DIM,), jnp.float32), 0.5, 1.5),
        "doc_starts": draw_doc_starts(jax.random.fold_in(jax.random.fold_in(streams_of[11], part), 71), part),
        "block_order": draw_block_order(jax.random.fold_in(jax.random.fold_in(streams_of[11], part), 71), part),
    }


highest = lax.Precision.HIGHEST

def product(form, left, right):
    return jnp.einsum(form, left.astype(jnp.float32), right.astype(jnp.float32), precision=highest)

def link_maps(earlier, current):
    decay_one, state_one = earlier
    decay_two, state_two = current
    return (decay_one * decay_two, decay_two[..., None, None] * state_one + state_two)

def group_terms(inputs, step_size, decay_speed, scores, write_vector, keep_mask, group_size):
    length, local_heads, head_width = inputs.shape
    group_count = length // group_size
    blocked = inputs.reshape(group_count, group_size, local_heads, head_width)
    steps_blocked = step_size.reshape(group_count, group_size, local_heads).transpose(0, 2, 1)
    cumulative = jnp.cumsum(-steps_blocked * decay_speed[None, :, None], axis=2)
    row_labels = lax.broadcasted_iota(jnp.int32, (group_size, group_size), 0)
    col_ids = lax.broadcasted_iota(jnp.int32, (group_size, group_size), 1)
    gap_log = cumulative[:, :, :, None] - cumulative[:, :, None, :]
    decays = jnp.exp(jnp.where(row_labels >= col_ids, gap_log, -jnp.inf))
    weight = (scores[:, None, :, :] * decays * steps_blocked[:, :, None, :]).astype(jnp.bfloat16)
    local_out = product('chij,cjhp->cihp', weight, blocked)
    last_cum = cumulative[:, :, -1]
    tail_decay = jnp.exp(last_cum[:, :, None] - cumulative) * steps_blocked
    scaled = (blocked.astype(jnp.float32) * tail_decay.transpose(0, 2, 1)[..., None]).astype(jnp.bfloat16)
    write_blocked = write_vector.reshape(group_count, group_size, -1)
    states = product('cjhp,cjn->chpn', scaled, write_blocked)
    factor = jnp.exp(last_cum) * keep_mask[:, None]
    scan_decay, scan_state = lax.associative_scan(link_maps, (factor, states))
    return (local_out, cumulative, scan_decay, scan_state)

def finish_groups(local_out, cumulative, scan_decay, scan_state, keep_mask, read_vector, starting_entry, inputs, skip_gain):
    group_count, group_size, local_heads, head_width = local_out.shape
    prior_decay = jnp.concatenate([jnp.ones((1, local_heads), jnp.float32), scan_decay[:-1]], 0)
    prior_state = jnp.concatenate([jnp.zeros((1,) + scan_state.shape[1:], jnp.float32), scan_state[:-1]], 0)
    entering = keep_mask[:, None, None, None] * (prior_decay[:, :, None, None] * starting_entry[None] + prior_state)
    read_blocked = read_vector.reshape(group_count, group_size, -1)
    carried = product('cin,chpn->cihp', read_blocked, entering)
    carried = carried * jnp.exp(cumulative).transpose(0, 2, 1)[..., None]
    blocked = inputs.reshape(local_out.shape).astype(jnp.float32)
    result = local_out + carried + skip_gain[None, None, :, None] * blocked
    return result.reshape(group_count * group_size, local_heads * head_width)

def gated_norm(gated, norm_weight):
    values = gated.astype(jnp.float32)
    mean_square = lax.optimization_barrier(jnp.mean(values * values, axis=-1, keepdims=True))
    return (values * lax.rsqrt(mean_square + 1e-05) * norm_weight).astype(jnp.bfloat16)

def reference(head_input, gate_input, write_vector, read_vector, increment_preactivation, step_bias, decay_log, skip_gain, norm_weight, doc_starts, block_order):
    step_size = jax.nn.softplus(increment_preactivation.astype(jnp.float32) + step_bias)
    decay_speed = jnp.exp(decay_log)
    keep_mask = 1.0 - doc_starts.astype(jnp.float32)
    group_count = JOINED_TERMS // GROUP
    scores = product('cin,cjn->cij', read_vector.reshape(group_count, GROUP, -1), write_vector.reshape(group_count, GROUP, -1))
    per_head = head_input.reshape(JOINED_TERMS, HEADS, HEAD_DIM).transpose(1, 0, 2)[:, :, None, :]

    def one_head(pieces):
        inputs, head_steps, attention_forgetting, head_gain = pieces
        local_out, cumulative, scan_decay, scan_state = group_terms(inputs, head_steps[:, None], attention_forgetting[None], scores, write_vector, keep_mask, GROUP)
        starting_entry = jnp.zeros((1, HEAD_DIM, STATE), jnp.float32)
        return finish_groups(local_out, cumulative, scan_decay, scan_state, keep_mask, read_vector, starting_entry, inputs, head_gain[None])
    outputs = lax.map(one_head, (per_head, step_size.T, decay_speed, skip_gain))
    combined = outputs.transpose(1, 0, 2).reshape(JOINED_TERMS, HEADS * HEAD_DIM)
    gated = (combined * jax.nn.silu(gate_input.astype(jnp.float32))).astype(jnp.bfloat16)
    normed = gated_norm(gated, norm_weight)
    return normed.reshape(group_count, GROUP, -1)[block_order].reshape(JOINED_TERMS, HEADS * HEAD_DIM)
```

```python
import functools

import jax
import jax.numpy as jnp
from jax import lax
from jax.experimental import pallas as pl
from jax.experimental.pallas import tpu as pltpu
from jax.sharding import PartitionSpec as P

HEAD_DIM = 64
GROUP = 128
CHUNK = 8
WIDE = CHUNK * HEAD_DIM
EXTRA = 16

highest = lax.Precision.HIGHEST
VM = pl.BlockSpec(memory_space=pltpu.VMEM)
SM = pl.BlockSpec(memory_space=pltpu.SMEM)


def transposed(v):
    rows, cols = v.shape
    if cols < 128:
        v = jnp.concatenate([v, jnp.zeros((rows, 128 - cols), v.dtype)], axis=1)
    return v.T[:cols]


def lower_mask():
    row = lax.broadcasted_iota(jnp.int32, (GROUP, GROUP), 0)
    col = lax.broadcasted_iota(jnp.int32, (GROUP, GROUP), 1)
    return row >= col


def step_terms(logit_ref, bias_ref, dlog_ref):
    v = logit_ref[...].astype(jnp.float32) + bias_ref[...]
    dt = jnp.maximum(v, 0.0) + jnp.log(1.0 + jnp.exp(-jnp.abs(v)))
    return dt, -dt * jnp.exp(dlog_ref[...])


def spread(v):
    rows = v.shape[0]
    first = lax.broadcasted_iota(jnp.int32, (rows, 128), 1) < HEAD_DIM
    return jnp.concatenate(
        [
            jnp.where(first, v[:, k : k + 1], v[:, k + 1 : k + 2])
            for k in range(0, CHUNK, 2)
        ],
        axis=1,
    )


def prepare(logit_ref, bias_ref, dlog_ref, write_ref, cum_s, dt_s, write_t):
    heads = bias_ref.shape[1]
    dt, fall = step_terms(logit_ref, bias_ref, dlog_ref)
    tri = lower_mask().astype(jnp.float32)
    cums = []
    for g in range(write_t.shape[0]):
        rows = slice(g * GROUP, (g + 1) * GROUP)
        cum = jnp.dot(tri, fall[rows], precision=highest, preferred_element_type=jnp.float32)
        cums.append(cum)
        for c in range(heads // CHUNK):
            cum_s[g, c] = cum[:, c * CHUNK : (c + 1) * CHUNK]
            dt_s[g, c] = dt[rows, c * CHUNK : (c + 1) * CHUNK]
        write_t[g] = write_ref[rows, :].astype(jnp.float32).T.astype(jnp.bfloat16)
    return dt, cums


def group_state(g, c, x, cum_s, dt_s, write_t):
    cum = cum_s[g, c]
    last = cum[GROUP - 1 : GROUP]
    tail = jnp.exp(last - cum) * dt_s[g, c]
    scaled = (x.astype(jnp.float32) * spread(tail)).astype(jnp.bfloat16)
    state = jnp.dot(write_t[g], scaled, preferred_element_type=jnp.float32)
    return state, spread(jnp.exp(last))


def state_kernel(
    x_ref, logit_ref, write_ref, bias_ref, dlog_ref, starts_ref, order_ref, out_ref, cum_s, dt_s, write_t
):
    groups = write_t.shape[0]
    prepare(logit_ref, bias_ref, dlog_ref, write_ref, cum_s, dt_s, write_t)
    parts, _, width = out_ref.shape
    chunks = cum_s.shape[1]
    per = width // WIDE

    def one(c, carry):
        cols = pl.ds(pl.multiple_of(c * WIDE, WIDE), WIDE)
        total, decay = None, None
        for g in range(groups):
            x = x_ref[g * GROUP : (g + 1) * GROUP, cols]
            state, last = group_state(g, c, x, cum_s, dt_s, write_t)
            keep = 1.0 - starts_ref[g].astype(jnp.float32)
            factor = keep * last
            total = state if total is None else factor * total + state
            decay = factor if decay is None else factor * decay
        coarse = decay.astype(jnp.bfloat16)
        fine = (decay - coarse.astype(jnp.float32)).astype(jnp.bfloat16)
        row = lax.broadcasted_iota(jnp.int32, (EXTRA, WIDE), 0)
        lane = lax.broadcasted_iota(jnp.int32, (EXTRA, WIDE), 1)
        order = jnp.zeros((EXTRA, WIDE), jnp.float32)
        for g in range(groups):
            order = jnp.where(lane == g, order_ref[g].astype(jnp.float32), order)
        extra = jnp.where(
            row == 0,
            coarse.astype(jnp.float32),
            jnp.where(row == 1, fine.astype(jnp.float32), order),
        )
        full = jnp.concatenate([total, extra], axis=0).astype(jnp.bfloat16)
        if parts == 1:
            out_ref[0, :, cols] = full
        else:
            into = pl.ds(pl.multiple_of((c % per) * WIDE, WIDE), WIDE)
            out_ref[c // per, :, into] = full
        return carry

    lax.fori_loop(0, chunks, one, 0)


def scan_kernel(in_ref, out_ref):
    parts, _, width = in_ref.shape
    state = jnp.zeros((GROUP, width), jnp.float32)
    for s in range(parts):
        out_ref[s] = state.astype(jnp.bfloat16)
        extra = in_ref[s, GROUP : GROUP + EXTRA, :].astype(jnp.float32)
        decay = extra[0:1] + extra[1:2]
        state = decay * state + in_ref[s, :GROUP, :].astype(jnp.float32)


def gated_kernel(
    x_ref,
    gate_ref,
    logit_ref,
    write_ref,
    read_ref,
    entry_ref,
    bias_ref,
    dlog_ref,
    gain_ref,
    starts_ref,
    out_ref,
    cum_s,
    dt_s,
    write_t,
    cum_t,
    dt_t,
    gain_s,
    score_s,
):
    groups, chunks = cum_s.shape[:2]
    dt, cums = prepare(logit_ref, bias_ref, dlog_ref, write_ref, cum_s, dt_s, write_t)
    mask = lower_mask()
    for g in range(groups):
        rows = slice(g * GROUP, (g + 1) * GROUP)
        ct = transposed(cums[g])
        dtt = transposed(dt[rows])
        for c in range(chunks):
            cum_t[g, c] = ct[c * CHUNK : (c + 1) * CHUNK]
            dt_t[g, c] = dtt[c * CHUNK : (c + 1) * CHUNK]
        score = jnp.dot(read_ref[rows, :], write_t[g], preferred_element_type=jnp.float32)
        score_s[g] = jnp.where(mask, score, 0.0)
    for c in range(chunks):
        gain_s[c] = jnp.broadcast_to(gain_ref[:, c * CHUNK : (c + 1) * CHUNK], (8, CHUNK))
    parts, _, width = out_ref.shape
    per = width // WIDE
    first = lax.broadcasted_iota(jnp.int32, (GROUP, 128), 1) < HEAD_DIM

    def one(c, carry):
        cols = pl.ds(pl.multiple_of(c * WIDE, WIDE), WIDE)
        into = pl.ds(pl.multiple_of((c % per) * WIDE, WIDE), WIDE)
        if entry_ref.shape[0] == 1:
            state = entry_ref[0, :, cols].astype(jnp.float32)
        else:
            state = entry_ref[c // per, :, into].astype(jnp.float32)
        gain = spread(gain_s[c][0:1])
        for g in range(groups):
            rows = slice(g * GROUP, (g + 1) * GROUP)
            x = x_ref[rows, cols]
            keep = 1.0 - starts_ref[g].astype(jnp.float32)
            entering = (keep * state).astype(jnp.bfloat16)
            cum = cum_s[g, c]
            carried = jnp.dot(read_ref[rows, :], entering, preferred_element_type=jnp.float32)
            mixed = carried * spread(jnp.exp(cum)) + gain * x.astype(jnp.float32)
            score = score_s[g]
            ct, dtt = cum_t[g, c], dt_t[g, c]
            pieces = []
            for k in range(0, CHUNK, 2):
                pair = x[:, k * HEAD_DIM : (k + 2) * HEAD_DIM]
                both = []
                for h in (k, k + 1):
                    gap = cum[:, h : h + 1] - ct[h : h + 1]
                    weight = score * jnp.exp(jnp.minimum(gap, 0.0)) * dtt[h : h + 1]
                    both.append(
                        jnp.dot(weight.astype(jnp.bfloat16), pair, preferred_element_type=jnp.float32)
                    )
                pieces.append(jnp.where(first, both[0], both[1]))
            mixed = mixed + jnp.concatenate(pieces, axis=1)
            gate = gate_ref[rows, cols].astype(jnp.float32)
            gated = (mixed * (gate / (1.0 + jnp.exp(-gate)))).astype(jnp.bfloat16)
            if parts == 1:
                out_ref[0, rows, cols] = gated
            else:
                out_ref[c // per, rows, into] = gated
            if g + 1 < groups:
                own, last = group_state(g, c, x, cum_s, dt_s, write_t)
                state = keep * last * state + own
        return carry

    lax.fori_loop(0, chunks, one, 0)


def norm_kernel(in_ref, weight_ref, out_ref):
    parts, rows, width = in_ref.shape
    tile = 32

    def one(r, carry):
        at = pl.ds(pl.multiple_of(r * tile, tile), tile)
        total = jnp.zeros((tile, 1), jnp.float32)
        for s in range(parts):
            v = in_ref[s, at, :].astype(jnp.float32)
            total = total + jnp.sum(v * v, axis=1, keepdims=True)
        scale = lax.rsqrt(total * (1.0 / (parts * width)) + 1e-05)
        for s in range(parts):
            v = in_ref[s, at, :].astype(jnp.float32)
            w = weight_ref[:, s * width : (s + 1) * width]
            out_ref[at, s * width : (s + 1) * width] = (v * scale * w).astype(jnp.bfloat16)
        return carry

    lax.fori_loop(0, rows // tile, one, 0)


def local(
    head_input,
    gate_input,
    write_vector,
    read_vector,
    increment_preactivation,
    step_bias,
    decay_log,
    skip_gain,
    norm_weight,
    doc_starts,
    block_order,
):
    devices = lax.axis_size("ctx")
    rows, features = head_input.shape
    heads = step_bias.shape[0]
    groups = rows // GROUP
    chunks = heads // CHUNK
    width = features // devices
    state_size = write_vector.shape[1]
    direct = width % WIDE == 0
    parts = devices if direct else 1
    limit = pltpu.CompilerParams(vmem_limit_bytes=48 * 1024 * 1024)
    common = [
        pltpu.VMEM((groups, chunks, GROUP, CHUNK), jnp.float32),
        pltpu.VMEM((groups, chunks, GROUP, CHUNK), jnp.float32),
        pltpu.VMEM((groups, state_size, GROUP), jnp.bfloat16),
    ]
    bias, dlog, gain = (v.reshape(1, -1) for v in (step_bias, decay_log, skip_gain))

    def to_owners(v):
        if not direct:
            v = v.reshape(v.shape[1], devices, width).transpose(1, 0, 2)
        return lax.all_to_all(v, "ctx", split_axis=0, concat_axis=0, tiled=True)

    def joined(v):
        if not direct:
            v = v.transpose(1, 0, 2).reshape(1, v.shape[1], features)
        return v

    ends = pl.pallas_call(
        state_kernel,
        out_shape=jax.ShapeDtypeStruct((parts, state_size + EXTRA, features // parts), jnp.bfloat16),
        in_specs=[VM] * 5 + [SM] * 2,
        out_specs=VM,
        scratch_shapes=common,
        compiler_params=limit,
        name="end_states",
    )(head_input, increment_preactivation, write_vector, bias, dlog, doc_starts, block_order)
    ends = to_owners(ends)
    all_order = ends[:, state_size + 2, :groups].astype(jnp.int32).reshape(-1)
    entry = pl.pallas_call(
        scan_kernel,
        out_shape=jax.ShapeDtypeStruct((devices, state_size, width), jnp.bfloat16),
        in_specs=[VM],
        out_specs=VM,
        compiler_params=limit,
        name="scan_states",
    )(ends)
    entry = joined(lax.all_to_all(entry, "ctx", split_axis=0, concat_axis=0, tiled=True))
    gated = pl.pallas_call(
        gated_kernel,
        out_shape=jax.ShapeDtypeStruct((parts, rows, features // parts), jnp.bfloat16),
        in_specs=[VM] * 9 + [SM],
        out_specs=VM,
        scratch_shapes=common
        + [
            pltpu.VMEM((groups, chunks, CHUNK, GROUP), jnp.float32),
            pltpu.VMEM((groups, chunks, CHUNK, GROUP), jnp.float32),
            pltpu.VMEM((chunks, 8, CHUNK), jnp.float32),
            pltpu.VMEM((groups, GROUP, GROUP), jnp.float32),
        ],
        compiler_params=limit,
        name="gated",
    )(
        head_input,
        gate_input,
        increment_preactivation,
        write_vector,
        read_vector,
        entry,
        bias,
        dlog,
        gain,
        doc_starts,
    )
    gated = to_owners(gated)
    blocks = gated.reshape(devices * groups, GROUP, width)[all_order]
    packed = lax.all_to_all(
        blocks.reshape(devices, rows, width), "ctx", split_axis=0, concat_axis=0, tiled=True
    )
    return pl.pallas_call(
        norm_kernel,
        out_shape=jax.ShapeDtypeStruct((rows, features), jnp.bfloat16),
        in_specs=[VM] * 2,
        out_specs=VM,
        compiler_params=limit,
        name="norm",
    )(joined(packed), norm_weight.reshape(1, -1))


def solution(mesh):
    return jax.shard_map(
        local,
        mesh=mesh,
        in_specs=(
            P(("dp", "ctx"), None),
            P(("dp", "ctx"), None),
            P(("dp", "ctx"), None),
            P(("dp", "ctx"), None),
            P(("dp", "ctx"), None),
            P(),
            P(),
            P(),
            P(),
            P(("dp", "ctx")),
            P(("dp", "ctx")),
        ),
        out_specs=P(("dp", "ctx"), None),
        check_vma=False,
    )
```

```python
import functools

import jax
import jax.numpy as jnp
from jax import lax
from jax.experimental import pallas as pl
from jax.experimental.pallas import tpu as pltpu
from jax.sharding import PartitionSpec as P

HEAD_DIM = 64
GROUP = 128
CHUNK = 8
WIDE = CHUNK * HEAD_DIM
EXTRA = 16

highest = lax.Precision.HIGHEST
VM = pl.BlockSpec(memory_space=pltpu.VMEM)
SM = pl.BlockSpec(memory_space=pltpu.SMEM)


def transposed(v):
    rows, cols = v.shape
    if cols < 128:
        v = jnp.concatenate([v, jnp.zeros((rows, 128 - cols), v.dtype)], axis=1)
    return v.T[:cols]


def lower_mask():
    row = lax.broadcasted_iota(jnp.int32, (GROUP, GROUP), 0)
    col = lax.broadcasted_iota(jnp.int32, (GROUP, GROUP), 1)
    return row >= col


def step_terms(logit_ref, bias_ref, dlog_ref):
    v = logit_ref[...].astype(jnp.float32) + bias_ref[...]
    dt = jnp.maximum(v, 0.0) + jnp.log(1.0 + jnp.exp(-jnp.abs(v)))
    return dt, -dt * jnp.exp(dlog_ref[...])


def spread(v):
    rows = v.shape[0]
    first = lax.broadcasted_iota(jnp.int32, (rows, 128), 1) < HEAD_DIM
    return jnp.concatenate(
        [
            jnp.where(first, v[:, k : k + 1], v[:, k + 1 : k + 2])
            for k in range(0, CHUNK, 2)
        ],
        axis=1,
    )


def prepare(logit_ref, bias_ref, dlog_ref, write_ref, cum_s, dt_s, write_t):
    heads = bias_ref.shape[1]
    dt, fall = step_terms(logit_ref, bias_ref, dlog_ref)
    tri = lower_mask().astype(jnp.float32)
    cums = []
    for g in range(write_t.shape[0]):
        rows = slice(g * GROUP, (g + 1) * GROUP)
        cum = jnp.dot(tri, fall[rows], precision=highest, preferred_element_type=jnp.float32)
        cums.append(cum)
        for c in range(heads // CHUNK):
            cum_s[g, c] = cum[:, c * CHUNK : (c + 1) * CHUNK]
            dt_s[g, c] = dt[rows, c * CHUNK : (c + 1) * CHUNK]
        write_t[g] = write_ref[rows, :].astype(jnp.float32).T.astype(jnp.bfloat16)
    return dt, cums


def group_state(g, c, x, cum_s, dt_s, write_t):
    cum = cum_s[g, c]
    last = cum[GROUP - 1 : GROUP]
    tail = jnp.exp(last - cum) * dt_s[g, c]
    scaled = (x.astype(jnp.float32) * spread(tail)).astype(jnp.bfloat16)
    state = jnp.dot(write_t[g], scaled, preferred_element_type=jnp.float32)
    return state, spread(jnp.exp(last))


def state_kernel(
    x_ref, logit_ref, write_ref, bias_ref, dlog_ref, starts_ref, order_ref, out_ref, cum_s, dt_s, write_t
):
    groups = write_t.shape[0]
    prepare(logit_ref, bias_ref, dlog_ref, write_ref, cum_s, dt_s, write_t)
    parts, _, width = out_ref.shape
    chunks = cum_s.shape[1]
    per = width // WIDE

    def one(c, carry):
        cols = pl.ds(pl.multiple_of(c * WIDE, WIDE), WIDE)
        total, decay = None, None
        for g in range(groups):
            x = x_ref[g * GROUP : (g + 1) * GROUP, cols]
            state, last = group_state(g, c, x, cum_s, dt_s, write_t)
            keep = 1.0 - starts_ref[g].astype(jnp.float32)
            factor = keep * last
            total = state if total is None else factor * total + state
            decay = factor if decay is None else factor * decay
        coarse = decay.astype(jnp.bfloat16)
        fine = (decay - coarse.astype(jnp.float32)).astype(jnp.bfloat16)
        row = lax.broadcasted_iota(jnp.int32, (EXTRA, WIDE), 0)
        lane = lax.broadcasted_iota(jnp.int32, (EXTRA, WIDE), 1)
        order = jnp.zeros((EXTRA, WIDE), jnp.float32)
        for g in range(groups):
            order = jnp.where(lane == g, order_ref[g].astype(jnp.float32), order)
        extra = jnp.where(
            row == 0,
            coarse.astype(jnp.float32),
            jnp.where(row == 1, fine.astype(jnp.float32), order),
        )
        full = jnp.concatenate([total, extra], axis=0).astype(jnp.bfloat16)
        if parts == 1:
            out_ref[0, :, cols] = full
        else:
            into = pl.ds(pl.multiple_of((c % per) * WIDE, WIDE), WIDE)
            out_ref[c // per, :, into] = full
        return carry

    lax.fori_loop(0, chunks, one, 0)


def scan_kernel(in_ref, out_ref):
    parts, _, width = in_ref.shape
    state = jnp.zeros((GROUP, width), jnp.float32)
    for s in range(parts):
        out_ref[s] = state.astype(jnp.bfloat16)
        extra = in_ref[s, GROUP : GROUP + EXTRA, :].astype(jnp.float32)
        decay = extra[0:1] + extra[1:2]
        state = decay * state + in_ref[s, :GROUP, :].astype(jnp.float32)


def gated_setup(
    logit_ref, bias_ref, dlog_ref, write_ref, read_ref, gain_ref, cum_s, dt_s, write_t, cum_t, dt_t, gain_s, score_s
):
    groups, chunks = cum_s.shape[:2]
    dt, cums = prepare(logit_ref, bias_ref, dlog_ref, write_ref, cum_s, dt_s, write_t)
    mask = lower_mask()
    for g in range(groups):
        rows = slice(g * GROUP, (g + 1) * GROUP)
        ct = transposed(cums[g])
        dtt = transposed(dt[rows])
        for c in range(chunks):
            cum_t[g, c] = ct[c * CHUNK : (c + 1) * CHUNK]
            dt_t[g, c] = dtt[c * CHUNK : (c + 1) * CHUNK]
        score = jnp.dot(read_ref[rows, :], write_t[g], preferred_element_type=jnp.float32)
        score_s[g] = jnp.where(mask, score, 0.0)
    for c in range(chunks):
        gain_s[c] = jnp.broadcast_to(gain_ref[:, c * CHUNK : (c + 1) * CHUNK], (8, CHUNK))


def gated_chunk(
    c, state, put, x_ref, gate_ref, read_ref, starts_ref, cum_s, dt_s, write_t, cum_t, dt_t, gain_s, score_s
):
    groups = cum_s.shape[0]
    first = lax.broadcasted_iota(jnp.int32, (GROUP, 128), 1) < HEAD_DIM
    cols = pl.ds(pl.multiple_of(c * WIDE, WIDE), WIDE)
    gain = spread(gain_s[c][0:1])
    for g in range(groups):
        rows = slice(g * GROUP, (g + 1) * GROUP)
        x = x_ref[rows, cols]
        keep = 1.0 - starts_ref[g].astype(jnp.float32)
        entering = (keep * state).astype(jnp.bfloat16)
        cum = cum_s[g, c]
        carried = jnp.dot(read_ref[rows, :], entering, preferred_element_type=jnp.float32)
        mixed = carried * spread(jnp.exp(cum)) + gain * x.astype(jnp.float32)
        score = score_s[g]
        ct, dtt = cum_t[g, c], dt_t[g, c]
        pieces = []
        for k in range(0, CHUNK, 2):
            pair = x[:, k * HEAD_DIM : (k + 2) * HEAD_DIM]
            both = []
            for h in (k, k + 1):
                gap = cum[:, h : h + 1] - ct[h : h + 1]
                weight = score * jnp.exp(jnp.minimum(gap, 0.0)) * dtt[h : h + 1]
                both.append(
                    jnp.dot(weight.astype(jnp.bfloat16), pair, preferred_element_type=jnp.float32)
                )
            pieces.append(jnp.where(first, both[0], both[1]))
        mixed = mixed + jnp.concatenate(pieces, axis=1)
        gate = gate_ref[rows, cols].astype(jnp.float32)
        put(g, (mixed * (gate / (1.0 + jnp.exp(-gate)))).astype(jnp.bfloat16))
        if g + 1 < groups:
            own, last = group_state(g, c, x, cum_s, dt_s, write_t)
            state = keep * last * state + own


def gated_kernel(
    x_ref,
    gate_ref,
    logit_ref,
    write_ref,
    read_ref,
    entry_ref,
    bias_ref,
    dlog_ref,
    gain_ref,
    starts_ref,
    out_ref,
    *scratch,
):
    gated_setup(logit_ref, bias_ref, dlog_ref, write_ref, read_ref, gain_ref, *scratch)
    parts, _, width = out_ref.shape
    chunks = scratch[0].shape[1]
    per = width // WIDE

    def one(c, carry):
        cols = pl.ds(pl.multiple_of(c * WIDE, WIDE), WIDE)
        into = pl.ds(pl.multiple_of((c % per) * WIDE, WIDE), WIDE)
        if parts == 1:
            state = entry_ref[0, :, cols].astype(jnp.float32)
        else:
            state = entry_ref[c // per, :, into].astype(jnp.float32)

        def put(g, value):
            rows = slice(g * GROUP, (g + 1) * GROUP)
            if parts == 1:
                out_ref[0, rows, cols] = value
            else:
                out_ref[c // per, rows, into] = value

        gated_chunk(c, state, put, x_ref, gate_ref, read_ref, starts_ref, *scratch)
        return carry

    lax.fori_loop(0, chunks, one, 0)


def fused_kernel(
    n,
    x_ref,
    gate_ref,
    logit_ref,
    write_ref,
    read_ref,
    bias_ref,
    dlog_ref,
    gain_ref,
    weight_ref,
    starts_ref,
    order_ref,
    out_ref,
    fin,
    fout,
    total_s,
    decay_s,
    made,
    got,
    stage,
    final,
    chain_send,
    chain_recv,
    send1,
    recv1,
    send2,
    recv2,
    *scratch,
):
    cum_s, dt_s, write_t = scratch[:3]
    groups = cum_s.shape[0]
    me = lax.axis_index("ctx")
    offsets = sorted(range(1, n), key=lambda k: abs(k - n // 2))
    barrier = pltpu.get_barrier_semaphore()
    for off in range(1, n):
        pl.semaphore_signal(
            barrier, inc=1, device_id={"ctx": lax.rem(me + off, n)}, device_id_type=pl.DeviceIdType.MESH
        )
    gated_setup(logit_ref, bias_ref, dlog_ref, write_ref, read_ref, gain_ref, *scratch)

    def ends(c, carry):
        cols = pl.ds(pl.multiple_of(c * WIDE, WIDE), WIDE)
        total, decay = None, None
        for g in range(groups):
            x = x_ref[g * GROUP : (g + 1) * GROUP, cols]
            state, last = group_state(g, c, x, cum_s, dt_s, write_t)
            factor = (1.0 - starts_ref[g].astype(jnp.float32)) * last
            total = state if total is None else factor * total + state
            decay = factor if decay is None else factor * decay
        total_s[c] = total
        decay_s[c] = jnp.broadcast_to(decay, (8, WIDE))
        return carry

    lax.fori_loop(0, n, ends, 0)

    @pl.when(me == 0)
    def _():
        fin[...] = jnp.zeros_like(fin)

    pl.semaphore_wait(barrier, n - 1)

    def chain(c):
        return pltpu.make_async_remote_copy(
            src_ref=fout.at[c],
            dst_ref=fin.at[c],
            send_sem=chain_send.at[c],
            recv_sem=chain_recv.at[c],
            device_id={"ctx": lax.rem(me + 1, n)},
            device_id_type=pl.DeviceIdType.MESH,
        )

    def outward(source, target, sends, recvs, there, slot):
        return pltpu.make_async_remote_copy(
            src_ref=source.at[there],
            dst_ref=target.at[pl.ds(slot * groups, groups)] if target is got else target.at[slot],
            send_sem=sends.at[there],
            recv_sem=recvs.at[slot],
            device_id={"ctx": there},
            device_id_type=pl.DeviceIdType.MESH,
        )

    def one(c, carry):
        @pl.when(me > 0)
        def _():
            chain(c).wait_recv()

        state = fin[c].astype(jnp.float32)

        @pl.when(me < n - 1)
        def _():
            fout[c] = (decay_s[c][0:1] * state + total_s[c]).astype(jnp.bfloat16)
            chain(c).start()

        def put(g, value):
            made[c, g] = value

        gated_chunk(c, state, put, x_ref, gate_ref, read_ref, starts_ref, *scratch)

        @pl.when(c != me)
        def _():
            outward(made, got, send1, recv1, c, me).start()

        @pl.when(c == me)
        def _():
            for g in range(groups):
                got[me * groups + g] = made[c, g]

        return carry

    lax.fori_loop(0, n, one, 0)
    for off in offsets:
        there = lax.rem(me + off, n)
        outward(made, got, send1, recv1, there, there).wait_recv()
    for off in offsets:
        there = lax.rem(me + off, n)
        for g in range(groups):
            stage[there, g] = got[order_ref[there * groups + g]]
        outward(stage, final, send2, recv2, there, me).start()
    for g in range(groups):
        final[me, g] = got[order_ref[me * groups + g]]

    @pl.when(me < n - 1)
    def _():
        for c in range(n):
            chain(c).wait_send()

    for off in offsets:
        there = lax.rem(me + off, n)
        outward(made, got, send1, recv1, there, there).wait_send()
        outward(stage, final, send2, recv2, there, there).wait_send()
    for off in offsets:
        there = lax.rem(me + off, n)
        outward(stage, final, send2, recv2, there, there).wait_recv()
    tile = 32
    for g in range(groups):

        def norm(r, carry):
            at = pl.ds(pl.multiple_of(r * tile, tile), tile)
            total = jnp.zeros((tile, 1), jnp.float32)
            for s in range(n):
                v = final[s, g, at, :].astype(jnp.float32)
                total = total + jnp.sum(v * v, axis=1, keepdims=True)
            scale = lax.rsqrt(total * (1.0 / (n * WIDE)) + 1e-05)
            for s in range(n):
                v = final[s, g, at, :].astype(jnp.float32)
                w = weight_ref[:, s * WIDE : (s + 1) * WIDE]
                into = pl.ds(pl.multiple_of(g * GROUP + r * tile, tile), tile)
                out_ref[into, s * WIDE : (s + 1) * WIDE] = (v * scale * w).astype(jnp.bfloat16)
            return carry

        lax.fori_loop(0, GROUP // tile, norm, 0)


def norm_kernel(in_ref, weight_ref, out_ref):
    parts, rows, width = in_ref.shape
    tile = 32

    def one(r, carry):
        at = pl.ds(pl.multiple_of(r * tile, tile), tile)
        total = jnp.zeros((tile, 1), jnp.float32)
        for s in range(parts):
            v = in_ref[s, at, :].astype(jnp.float32)
            total = total + jnp.sum(v * v, axis=1, keepdims=True)
        scale = lax.rsqrt(total * (1.0 / (parts * width)) + 1e-05)
        for s in range(parts):
            v = in_ref[s, at, :].astype(jnp.float32)
            w = weight_ref[:, s * width : (s + 1) * width]
            out_ref[at, s * width : (s + 1) * width] = (v * scale * w).astype(jnp.bfloat16)
        return carry

    lax.fori_loop(0, rows // tile, one, 0)


def local(
    head_input,
    gate_input,
    write_vector,
    read_vector,
    increment_preactivation,
    step_bias,
    decay_log,
    skip_gain,
    norm_weight,
    doc_starts,
    block_order,
):
    devices = lax.axis_size("ctx")
    rows, features = head_input.shape
    heads = step_bias.shape[0]
    groups = rows // GROUP
    chunks = heads // CHUNK
    width = features // devices
    state_size = write_vector.shape[1]
    direct = width % WIDE == 0
    parts = devices if direct else 1
    limit = pltpu.CompilerParams(vmem_limit_bytes=48 * 1024 * 1024)
    common = [
        pltpu.VMEM((groups, chunks, GROUP, CHUNK), jnp.float32),
        pltpu.VMEM((groups, chunks, GROUP, CHUNK), jnp.float32),
        pltpu.VMEM((groups, state_size, GROUP), jnp.bfloat16),
    ]
    more = [
        pltpu.VMEM((groups, chunks, CHUNK, GROUP), jnp.float32),
        pltpu.VMEM((groups, chunks, CHUNK, GROUP), jnp.float32),
        pltpu.VMEM((chunks, 8, CHUNK), jnp.float32),
        pltpu.VMEM((groups, GROUP, GROUP), jnp.float32),
    ]
    bias, dlog, gain = (v.reshape(1, -1) for v in (step_bias, decay_log, skip_gain))

    def to_owners(v):
        if not direct:
            v = v.reshape(v.shape[1], devices, width).transpose(1, 0, 2)
        return lax.all_to_all(v, "ctx", split_axis=0, concat_axis=0, tiled=True)

    def joined(v):
        if not direct:
            v = v.transpose(1, 0, 2).reshape(1, v.shape[1], features)
        return v

    if width == WIDE:
        all_order = lax.all_gather(block_order, "ctx", axis=0, tiled=True)
        slab = (devices, groups, GROUP, WIDE)
        return pl.pallas_call(
            functools.partial(fused_kernel, devices),
            out_shape=jax.ShapeDtypeStruct((rows, features), jnp.bfloat16),
            in_specs=[VM] * 9 + [SM] * 2,
            out_specs=VM,
            scratch_shapes=[
                pltpu.VMEM((devices, state_size, WIDE), jnp.bfloat16),
                pltpu.VMEM((devices, state_size, WIDE), jnp.bfloat16),
                pltpu.VMEM((devices, state_size, WIDE), jnp.float32),
                pltpu.VMEM((devices, 8, WIDE), jnp.float32),
                pltpu.VMEM(slab, jnp.bfloat16),
                pltpu.VMEM((devices * groups, GROUP, WIDE), jnp.bfloat16),
                pltpu.VMEM(slab, jnp.bfloat16),
                pltpu.VMEM(slab, jnp.bfloat16),
            ]
            + [pltpu.SemaphoreType.DMA((devices,))] * 6
            + common
            + more,
            compiler_params=pltpu.CompilerParams(
                collective_id=0, has_side_effects=True, vmem_limit_bytes=56 * 1024 * 1024
            ),
            name="fused",
        )(
            head_input,
            gate_input,
            increment_preactivation,
            write_vector,
            read_vector,
            bias,
            dlog,
            gain,
            norm_weight.reshape(1, -1),
            doc_starts,
            all_order,
        )

    ends = pl.pallas_call(
        state_kernel,
        out_shape=jax.ShapeDtypeStruct((parts, state_size + EXTRA, features // parts), jnp.bfloat16),
        in_specs=[VM] * 5 + [SM] * 2,
        out_specs=VM,
        scratch_shapes=common,
        compiler_params=limit,
        name="end_states",
    )(head_input, increment_preactivation, write_vector, bias, dlog, doc_starts, block_order)
    ends = to_owners(ends)
    all_order = ends[:, state_size + 2, :groups].astype(jnp.int32).reshape(-1)
    entry = pl.pallas_call(
        scan_kernel,
        out_shape=jax.ShapeDtypeStruct((devices, state_size, width), jnp.bfloat16),
        in_specs=[VM],
        out_specs=VM,
        compiler_params=limit,
        name="scan_states",
    )(ends)
    entry = joined(lax.all_to_all(entry, "ctx", split_axis=0, concat_axis=0, tiled=True))
    gated = pl.pallas_call(
        gated_kernel,
        out_shape=jax.ShapeDtypeStruct((parts, rows, features // parts), jnp.bfloat16),
        in_specs=[VM] * 9 + [SM],
        out_specs=VM,
        scratch_shapes=common
        + more,
        compiler_params=limit,
        name="gated",
    )(
        head_input,
        gate_input,
        increment_preactivation,
        write_vector,
        read_vector,
        entry,
        bias,
        dlog,
        gain,
        doc_starts,
    )
    gated = to_owners(gated)
    blocks = gated.reshape(devices * groups, GROUP, width)[all_order]
    packed = lax.all_to_all(
        blocks.reshape(devices, rows, width), "ctx", split_axis=0, concat_axis=0, tiled=True
    )
    return pl.pallas_call(
        norm_kernel,
        out_shape=jax.ShapeDtypeStruct((rows, features), jnp.bfloat16),
        in_specs=[VM] * 2,
        out_specs=VM,
        compiler_params=limit,
        name="norm",
    )(joined(packed), norm_weight.reshape(1, -1))


def solution(mesh):
    return jax.shard_map(
        local,
        mesh=mesh,
        in_specs=(
            P(("dp", "ctx"), None),
            P(("dp", "ctx"), None),
            P(("dp", "ctx"), None),
            P(("dp", "ctx"), None),
            P(("dp", "ctx"), None),
            P(),
            P(),
            P(),
            P(),
            P(("dp", "ctx")),
            P(("dp", "ctx")),
        ),
        out_specs=P(("dp", "ctx"), None),
        check_vma=False,
    )
```

```python
import functools

import jax
import jax.numpy as jnp
from jax import lax
from jax.experimental import pallas as pl
from jax.experimental.pallas import tpu as pltpu
from jax.sharding import PartitionSpec as P

HEAD_DIM = 64
GROUP = 128
CHUNK = 8
WIDE = CHUNK * HEAD_DIM
EXTRA = 16

highest = lax.Precision.HIGHEST
VM = pl.BlockSpec(memory_space=pltpu.VMEM)
SM = pl.BlockSpec(memory_space=pltpu.SMEM)


def transposed(v):
    rows, cols = v.shape
    if cols < 128:
        v = jnp.concatenate([v, jnp.zeros((rows, 128 - cols), v.dtype)], axis=1)
    return v.T[:cols]


def lower_mask():
    row = lax.broadcasted_iota(jnp.int32, (GROUP, GROUP), 0)
    col = lax.broadcasted_iota(jnp.int32, (GROUP, GROUP), 1)
    return row >= col


def step_terms(logit_ref, bias_ref, dlog_ref):
    v = logit_ref[...].astype(jnp.float32) + bias_ref[...]
    dt = jnp.maximum(v, 0.0) + jnp.log(1.0 + jnp.exp(-jnp.abs(v)))
    return dt, -dt * jnp.exp(dlog_ref[...])


def spread(v):
    rows = v.shape[0]
    first = lax.broadcasted_iota(jnp.int32, (rows, 128), 1) < HEAD_DIM
    return jnp.concatenate(
        [
            jnp.where(first, v[:, k : k + 1], v[:, k + 1 : k + 2])
            for k in range(0, CHUNK, 2)
        ],
        axis=1,
    )


def prepare(logit_ref, bias_ref, dlog_ref, write_ref, cum_s, dt_s, write_t):
    heads = bias_ref.shape[1]
    dt, fall = step_terms(logit_ref, bias_ref, dlog_ref)
    tri = lower_mask().astype(jnp.float32)
    cums = []
    for g in range(write_t.shape[0]):
        rows = slice(g * GROUP, (g + 1) * GROUP)
        cum = jnp.dot(tri, fall[rows], precision=highest, preferred_element_type=jnp.float32)
        cums.append(cum)
        for c in range(heads // CHUNK):
            cum_s[g, c] = cum[:, c * CHUNK : (c + 1) * CHUNK]
            dt_s[g, c] = dt[rows, c * CHUNK : (c + 1) * CHUNK]
        write_t[g] = write_ref[rows, :].astype(jnp.float32).T.astype(jnp.bfloat16)
    return dt, cums


def group_state(g, c, x, cum_s, dt_s, write_t):
    cum = cum_s[g, c]
    last = cum[GROUP - 1 : GROUP]
    tail = jnp.exp(last - cum) * dt_s[g, c]
    scaled = (x.astype(jnp.float32) * spread(tail)).astype(jnp.bfloat16)
    state = jnp.dot(write_t[g], scaled, preferred_element_type=jnp.float32)
    return state, spread(jnp.exp(last))


def state_kernel(
    x_ref, logit_ref, write_ref, bias_ref, dlog_ref, starts_ref, order_ref, out_ref, cum_s, dt_s, write_t
):
    groups = write_t.shape[0]
    prepare(logit_ref, bias_ref, dlog_ref, write_ref, cum_s, dt_s, write_t)
    parts, _, width = out_ref.shape
    chunks = cum_s.shape[1]
    per = width // WIDE

    def one(c, carry):
        cols = pl.ds(pl.multiple_of(c * WIDE, WIDE), WIDE)
        total, decay = None, None
        for g in range(groups):
            x = x_ref[g * GROUP : (g + 1) * GROUP, cols]
            state, last = group_state(g, c, x, cum_s, dt_s, write_t)
            keep = 1.0 - starts_ref[g].astype(jnp.float32)
            factor = keep * last
            total = state if total is None else factor * total + state
            decay = factor if decay is None else factor * decay
        coarse = decay.astype(jnp.bfloat16)
        fine = (decay - coarse.astype(jnp.float32)).astype(jnp.bfloat16)
        row = lax.broadcasted_iota(jnp.int32, (EXTRA, WIDE), 0)
        lane = lax.broadcasted_iota(jnp.int32, (EXTRA, WIDE), 1)
        order = jnp.zeros((EXTRA, WIDE), jnp.float32)
        for g in range(groups):
            order = jnp.where(lane == g, order_ref[g].astype(jnp.float32), order)
        extra = jnp.where(
            row == 0,
            coarse.astype(jnp.float32),
            jnp.where(row == 1, fine.astype(jnp.float32), order),
        )
        full = jnp.concatenate([total, extra], axis=0).astype(jnp.bfloat16)
        if parts == 1:
            out_ref[0, :, cols] = full
        else:
            into = pl.ds(pl.multiple_of((c % per) * WIDE, WIDE), WIDE)
            out_ref[c // per, :, into] = full
        return carry

    lax.fori_loop(0, chunks, one, 0)


def scan_kernel(in_ref, out_ref):
    parts, _, width = in_ref.shape
    state = jnp.zeros((GROUP, width), jnp.float32)
    for s in range(parts):
        out_ref[s] = state.astype(jnp.bfloat16)
        extra = in_ref[s, GROUP : GROUP + EXTRA, :].astype(jnp.float32)
        decay = extra[0:1] + extra[1:2]
        state = decay * state + in_ref[s, :GROUP, :].astype(jnp.float32)


def gated_setup(
    logit_ref, bias_ref, dlog_ref, write_ref, read_ref, gain_ref, cum_s, dt_s, write_t, cum_t, dt_t, gain_s, score_s
):
    groups, chunks = cum_s.shape[:2]
    dt, cums = prepare(logit_ref, bias_ref, dlog_ref, write_ref, cum_s, dt_s, write_t)
    mask = lower_mask()
    for g in range(groups):
        rows = slice(g * GROUP, (g + 1) * GROUP)
        ct = transposed(cums[g])
        dtt = transposed(dt[rows])
        for c in range(chunks):
            cum_t[g, c] = ct[c * CHUNK : (c + 1) * CHUNK]
            dt_t[g, c] = dtt[c * CHUNK : (c + 1) * CHUNK]
        score = jnp.dot(read_ref[rows, :], write_t[g], preferred_element_type=jnp.float32)
        score_s[g] = jnp.where(mask, score, 0.0)
    for c in range(chunks):
        gain_s[c] = jnp.broadcast_to(gain_ref[:, c * CHUNK : (c + 1) * CHUNK], (8, CHUNK))


def gated_chunk(
    c, state, put, x_ref, gate_ref, read_ref, starts_ref, cum_s, dt_s, write_t, cum_t, dt_t, gain_s, score_s
):
    groups = cum_s.shape[0]
    first = lax.broadcasted_iota(jnp.int32, (GROUP, 128), 1) < HEAD_DIM
    cols = pl.ds(pl.multiple_of(c * WIDE, WIDE), WIDE)
    gain = spread(gain_s[c][0:1])
    for g in range(groups):
        rows = slice(g * GROUP, (g + 1) * GROUP)
        x = x_ref[rows, cols]
        keep = 1.0 - starts_ref[g].astype(jnp.float32)
        entering = (keep * state).astype(jnp.bfloat16)
        cum = cum_s[g, c]
        carried = jnp.dot(read_ref[rows, :], entering, preferred_element_type=jnp.float32)
        mixed = carried * spread(jnp.exp(cum)) + gain * x.astype(jnp.float32)
        score = score_s[g]
        ct, dtt = cum_t[g, c], dt_t[g, c]
        pieces = []
        for k in range(0, CHUNK, 2):
            pair = x[:, k * HEAD_DIM : (k + 2) * HEAD_DIM]
            both = []
            for h in (k, k + 1):
                gap = cum[:, h : h + 1] - ct[h : h + 1]
                weight = score * jnp.exp(jnp.minimum(gap, 0.0)) * dtt[h : h + 1]
                both.append(
                    jnp.dot(weight.astype(jnp.bfloat16), pair, preferred_element_type=jnp.float32)
                )
            pieces.append(jnp.where(first, both[0], both[1]))
        mixed = mixed + jnp.concatenate(pieces, axis=1)
        gate = gate_ref[rows, cols].astype(jnp.float32)
        put(g, (mixed * (gate / (1.0 + jnp.exp(-gate)))).astype(jnp.bfloat16))
        if g + 1 < groups:
            own, last = group_state(g, c, x, cum_s, dt_s, write_t)
            state = keep * last * state + own


def gated_kernel(
    x_ref,
    gate_ref,
    logit_ref,
    write_ref,
    read_ref,
    entry_ref,
    bias_ref,
    dlog_ref,
    gain_ref,
    starts_ref,
    out_ref,
    *scratch,
):
    gated_setup(logit_ref, bias_ref, dlog_ref, write_ref, read_ref, gain_ref, *scratch)
    parts, _, width = out_ref.shape
    chunks = scratch[0].shape[1]
    per = width // WIDE

    def one(c, carry):
        cols = pl.ds(pl.multiple_of(c * WIDE, WIDE), WIDE)
        into = pl.ds(pl.multiple_of((c % per) * WIDE, WIDE), WIDE)
        if parts == 1:
            state = entry_ref[0, :, cols].astype(jnp.float32)
        else:
            state = entry_ref[c // per, :, into].astype(jnp.float32)

        def put(g, value):
            rows = slice(g * GROUP, (g + 1) * GROUP)
            if parts == 1:
                out_ref[0, rows, cols] = value
            else:
                out_ref[c // per, rows, into] = value

        gated_chunk(c, state, put, x_ref, gate_ref, read_ref, starts_ref, *scratch)
        return carry

    lax.fori_loop(0, chunks, one, 0)


def fused_kernel(
    n,
    x_ref,
    gate_ref,
    logit_ref,
    write_ref,
    read_ref,
    bias_ref,
    dlog_ref,
    gain_ref,
    weight_ref,
    starts_ref,
    order_ref,
    out_ref,
    fin,
    fout,
    total_s,
    decay_s,
    made,
    got,
    stage,
    final,
    chain_send,
    chain_recv,
    send1,
    recv1,
    send2,
    recv2,
    send3,
    recv3,
    order_all,
    order_s,
    order_sem,
    *scratch,
):
    cum_s, dt_s, write_t = scratch[:3]
    groups = cum_s.shape[0]
    me = lax.axis_index("ctx")
    offsets = range(1, n)
    half = n // 2
    mine = (me // half) * half
    other = half - mine

    def partner(k):
        far = 1 - k % 2
        return far * other + (1 - far) * mine + lax.rem(me + k // 2, half)

    barrier = pltpu.get_barrier_semaphore()
    for off in range(1, n):
        pl.semaphore_signal(
            barrier, inc=1, device_id={"ctx": lax.rem(me + off, n)}, device_id_type=pl.DeviceIdType.MESH
        )
    gated_setup(logit_ref, bias_ref, dlog_ref, write_ref, read_ref, gain_ref, *scratch)

    @pl.when(me == 0)
    def _():
        fin[...] = jnp.zeros_like(fin)

    def chain(c):
        return pltpu.make_async_remote_copy(
            src_ref=fout.at[c],
            dst_ref=fin.at[c],
            send_sem=chain_send.at[c],
            recv_sem=chain_recv.at[c],
            device_id={"ctx": lax.rem(me + 1, n)},
            device_id_type=pl.DeviceIdType.MESH,
        )

    def spread_order(there, slot):
        return pltpu.make_async_remote_copy(
            src_ref=order_ref,
            dst_ref=order_all.at[slot],
            send_sem=send3.at[there],
            recv_sem=recv3.at[slot],
            device_id={"ctx": there},
            device_id_type=pl.DeviceIdType.MESH,
        )

    def outward(source, target, sends, recvs, there, slot):
        return pltpu.make_async_remote_copy(
            src_ref=source.at[there],
            dst_ref=target.at[pl.ds(slot * groups, groups)] if target is got else target.at[slot],
            send_sem=sends.at[there],
            recv_sem=recvs.at[slot],
            device_id={"ctx": there},
            device_id_type=pl.DeviceIdType.MESH,
        )

    pl.semaphore_wait(barrier, n - 1)
    order_all[me] = order_ref[...]
    for off in offsets:
        spread_order(lax.rem(me + off, n), me).start()

    def ends(c, carry):
        cols = pl.ds(pl.multiple_of(c * WIDE, WIDE), WIDE)
        total, decay = None, None
        for g in range(groups):
            x = x_ref[g * GROUP : (g + 1) * GROUP, cols]
            state, last = group_state(g, c, x, cum_s, dt_s, write_t)
            factor = (1.0 - starts_ref[g].astype(jnp.float32)) * last
            total = state if total is None else factor * total + state
            decay = factor if decay is None else factor * decay
        total_s[c] = total
        decay_s[c] = jnp.broadcast_to(decay, (8, WIDE))

        @pl.when(me == 0)
        def _():
            fout[c] = total.astype(jnp.bfloat16)
            chain(c).start()

        return carry

    lax.fori_loop(0, n, ends, 0)

    def relay(c, carry):
        chain(c).wait_recv()

        @pl.when(me < n - 1)
        def _():
            state = fin[c].astype(jnp.float32)
            fout[c] = (decay_s[c][0:1] * state + total_s[c]).astype(jnp.bfloat16)
            chain(c).start()

        return carry

    @pl.when(me > 0)
    def _():
        lax.fori_loop(0, n, relay, 0)

    def one(k, carry):
        c = partner(k)
        state = fin[c].astype(jnp.float32)

        def put(g, value):
            made[c, g] = value

        gated_chunk(c, state, put, x_ref, gate_ref, read_ref, starts_ref, *scratch)

        @pl.when(c != me)
        def _():
            outward(made, got, send1, recv1, c, me).start()

        @pl.when(c == me)
        def _():
            for g in range(groups):
                got[me * groups + g] = made[c, g]

        return carry

    lax.fori_loop(0, n, one, 0)
    for off in offsets:
        there = lax.rem(me + off, n)
        spread_order(there, there).wait_recv()
    fetch = pltpu.make_async_copy(order_all, order_s, order_sem)
    fetch.start()
    fetch.wait()
    for off in offsets:
        there = lax.rem(me + off, n)
        outward(made, got, send1, recv1, there, there).wait_recv()

    def second(k, carry):
        there = partner(k)
        for g in range(groups):
            stage[there, g] = got[order_s[there, 0, g]]

        @pl.when(there != me)
        def _():
            outward(stage, final, send2, recv2, there, me).start()

        return carry

    lax.fori_loop(0, n, second, 0)
    for g in range(groups):
        final[me, g] = stage[me, g]

    @pl.when(me < n - 1)
    def _():
        for c in range(n):
            chain(c).wait_send()

    for off in offsets:
        there = lax.rem(me + off, n)
        outward(made, got, send1, recv1, there, there).wait_send()
        outward(stage, final, send2, recv2, there, there).wait_send()
        spread_order(there, there).wait_send()
    for off in offsets:
        there = lax.rem(me + off, n)
        outward(stage, final, send2, recv2, there, there).wait_recv()
    tile = 32
    for g in range(groups):

        def norm(r, carry):
            at = pl.ds(pl.multiple_of(r * tile, tile), tile)
            total = jnp.zeros((tile, 1), jnp.float32)
            for s in range(n):
                v = final[s, g, at, :].astype(jnp.float32)
                total = total + jnp.sum(v * v, axis=1, keepdims=True)
            scale = lax.rsqrt(total * (1.0 / (n * WIDE)) + 1e-05)
            for s in range(n):
                v = final[s, g, at, :].astype(jnp.float32)
                w = weight_ref[:, s * WIDE : (s + 1) * WIDE]
                into = pl.ds(pl.multiple_of(g * GROUP + r * tile, tile), tile)
                out_ref[into, s * WIDE : (s + 1) * WIDE] = (v * scale * w).astype(jnp.bfloat16)
            return carry

        lax.fori_loop(0, GROUP // tile, norm, 0)


def norm_kernel(in_ref, weight_ref, out_ref):
    parts, rows, width = in_ref.shape
    tile = 32

    def one(r, carry):
        at = pl.ds(pl.multiple_of(r * tile, tile), tile)
        total = jnp.zeros((tile, 1), jnp.float32)
        for s in range(parts):
            v = in_ref[s, at, :].astype(jnp.float32)
            total = total + jnp.sum(v * v, axis=1, keepdims=True)
        scale = lax.rsqrt(total * (1.0 / (parts * width)) + 1e-05)
        for s in range(parts):
            v = in_ref[s, at, :].astype(jnp.float32)
            w = weight_ref[:, s * width : (s + 1) * width]
            out_ref[at, s * width : (s + 1) * width] = (v * scale * w).astype(jnp.bfloat16)
        return carry

    lax.fori_loop(0, rows // tile, one, 0)


def local(
    head_input,
    gate_input,
    write_vector,
    read_vector,
    increment_preactivation,
    step_bias,
    decay_log,
    skip_gain,
    norm_weight,
    doc_starts,
    block_order,
):
    devices = lax.axis_size("ctx")
    rows, features = head_input.shape
    heads = step_bias.shape[0]
    groups = rows // GROUP
    chunks = heads // CHUNK
    width = features // devices
    state_size = write_vector.shape[1]
    direct = width % WIDE == 0
    parts = devices if direct else 1
    limit = pltpu.CompilerParams(vmem_limit_bytes=48 * 1024 * 1024)
    common = [
        pltpu.VMEM((groups, chunks, GROUP, CHUNK), jnp.float32),
        pltpu.VMEM((groups, chunks, GROUP, CHUNK), jnp.float32),
        pltpu.VMEM((groups, state_size, GROUP), jnp.bfloat16),
    ]
    more = [
        pltpu.VMEM((groups, chunks, CHUNK, GROUP), jnp.float32),
        pltpu.VMEM((groups, chunks, CHUNK, GROUP), jnp.float32),
        pltpu.VMEM((chunks, 8, CHUNK), jnp.float32),
        pltpu.VMEM((groups, GROUP, GROUP), jnp.float32),
    ]
    bias, dlog, gain = (v.reshape(1, -1) for v in (step_bias, decay_log, skip_gain))

    def to_owners(v):
        if not direct:
            v = v.reshape(v.shape[1], devices, width).transpose(1, 0, 2)
        return lax.all_to_all(v, "ctx", split_axis=0, concat_axis=0, tiled=True)

    def joined(v):
        if not direct:
            v = v.transpose(1, 0, 2).reshape(1, v.shape[1], features)
        return v

    if width == WIDE and devices % 2 == 0:
        order = jnp.broadcast_to(jnp.pad(block_order, (0, 128 - groups))[None], (8, 128))
        slab = (devices, groups, GROUP, WIDE)
        return pl.pallas_call(
            functools.partial(fused_kernel, devices),
            out_shape=jax.ShapeDtypeStruct((rows, features), jnp.bfloat16),
            in_specs=[VM] * 9 + [SM, VM],
            out_specs=VM,
            scratch_shapes=[
                pltpu.VMEM((devices, state_size, WIDE), jnp.bfloat16),
                pltpu.VMEM((devices, state_size, WIDE), jnp.bfloat16),
                pltpu.VMEM((devices, state_size, WIDE), jnp.float32),
                pltpu.VMEM((devices, 8, WIDE), jnp.float32),
                pltpu.VMEM(slab, jnp.bfloat16),
                pltpu.VMEM((devices * groups, GROUP, WIDE), jnp.bfloat16),
                pltpu.VMEM(slab, jnp.bfloat16),
                pltpu.VMEM(slab, jnp.bfloat16),
            ]
            + [pltpu.SemaphoreType.DMA((devices,))] * 8
            + [
                pltpu.VMEM((devices, 8, 128), jnp.int32),
                pltpu.SMEM((devices, 8, 128), jnp.int32),
                pltpu.SemaphoreType.DMA,
            ]
            + common
            + more,
            compiler_params=pltpu.CompilerParams(
                collective_id=0, has_side_effects=True, vmem_limit_bytes=56 * 1024 * 1024
            ),
            name="fused",
        )(
            head_input,
            gate_input,
            increment_preactivation,
            write_vector,
            read_vector,
            bias,
            dlog,
            gain,
            norm_weight.reshape(1, -1),
            doc_starts,
            order,
        )

    ends = pl.pallas_call(
        state_kernel,
        out_shape=jax.ShapeDtypeStruct((parts, state_size + EXTRA, features // parts), jnp.bfloat16),
        in_specs=[VM] * 5 + [SM] * 2,
        out_specs=VM,
        scratch_shapes=common,
        compiler_params=limit,
        name="end_states",
    )(head_input, increment_preactivation, write_vector, bias, dlog, doc_starts, block_order)
    ends = to_owners(ends)
    all_order = ends[:, state_size + 2, :groups].astype(jnp.int32).reshape(-1)
    entry = pl.pallas_call(
        scan_kernel,
        out_shape=jax.ShapeDtypeStruct((devices, state_size, width), jnp.bfloat16),
        in_specs=[VM],
        out_specs=VM,
        compiler_params=limit,
        name="scan_states",
    )(ends)
    entry = joined(lax.all_to_all(entry, "ctx", split_axis=0, concat_axis=0, tiled=True))
    gated = pl.pallas_call(
        gated_kernel,
        out_shape=jax.ShapeDtypeStruct((parts, rows, features // parts), jnp.bfloat16),
        in_specs=[VM] * 9 + [SM],
        out_specs=VM,
        scratch_shapes=common
        + more,
        compiler_params=limit,
        name="gated",
    )(
        head_input,
        gate_input,
        increment_preactivation,
        write_vector,
        read_vector,
        entry,
        bias,
        dlog,
        gain,
        doc_starts,
    )
    gated = to_owners(gated)
    blocks = gated.reshape(devices * groups, GROUP, width)[all_order]
    packed = lax.all_to_all(
        blocks.reshape(devices, rows, width), "ctx", split_axis=0, concat_axis=0, tiled=True
    )
    return pl.pallas_call(
        norm_kernel,
        out_shape=jax.ShapeDtypeStruct((rows, features), jnp.bfloat16),
        in_specs=[VM] * 2,
        out_specs=VM,
        compiler_params=limit,
        name="norm",
    )(joined(packed), norm_weight.reshape(1, -1))


def solution(mesh):
    return jax.shard_map(
        local,
        mesh=mesh,
        in_specs=(
            P(("dp", "ctx"), None),
            P(("dp", "ctx"), None),
            P(("dp", "ctx"), None),
            P(("dp", "ctx"), None),
            P(("dp", "ctx"), None),
            P(),
            P(),
            P(),
            P(),
            P(("dp", "ctx")),
            P(("dp", "ctx")),
        ),
        out_specs=P(("dp", "ctx"), None),
        check_vma=False,
    )
```
